256 devices in a mesh: member: 16 (over z, core), space: 16 (over x, y).
Axes of the slice: x: 4, y: 4, z: 8, core: 2. Of those that a mesh axis runs over, the one named last changes fastest.
Arguments:
- latents: bfloat16 [12288, 512], P('space'), may hold values from -6 to 6
- sample_perturbation: bfloat16 [48, 12288, 512], P('member', 'space'), may hold values from -6 to 6
- noise_table: float32 [64, 512], replicated, may hold values from 0.2 to 1.5
- member_seed: int32 [48], P('member'), may hold values from 0 to 63
- piece_arrangement: int32 [768], replicated, may hold values from 0 to 767, each once
- targets: bfloat16 [12288, 384], P('space'), may hold values from -4 to 4
- w_gate: bfloat16 [512, 1024], replicated, may hold values from -0.25 to 0.25
- w_up: bfloat16 [512, 1024], replicated, may hold values from -0.25 to 0.25
- lowering_matrix: bfloat16 [1024, 384], replicated, may hold values from -0.1875 to 0.1875
Outputs:
- latent_grad: float32 [12288, 512], P('space', 'member')
The draws below stay inside these ranges and needn't reach their ends.
Inputs may be any that keep to these rules, and one draw needn't show every extreme that they name: `piece_arrangement`: a permutation of the 768 positions of a tile, the same for every tile.
All inputs are finite; a program needn't handle non-finite values.
Results may differ from the reference program's by a relative error of at most 0.0019.
Values may be sent and summed in bfloat16 or wider, within the bound.
No kernel may reach another device: no remote copies, remote signals or barrier semaphores. Data moves between devices by JAX's collectives and lax.ppermute only.
A program may use at most 128 MiB of HBM per device.

```python
import jax
import jax.numpy as jnp
from jax import lax

LAT = 512
HID = 1024
RESULT_DIM = 384
PIECE_ITEMS = 8
TABLE = 64
REGION_ITEMS = 768
MEMBERS = 48
TOKENS = 12288


def touch_ends(values, own_key, smallest, largest):
    shape = values.shape
    place = [jax.random.randint(jax.random.fold_in(own_key, axis), (), 0, shape[axis]) for axis in range(len(shape))]
    values = values.at[tuple(place)].set(smallest)
    longest = shape.index(max(shape))
    place[longest] = (place[longest] + 1) % shape[longest]
    return values.at[tuple(place)].set(largest)


def block_levels(rng, shape, shards, least, largest):
    loudness, own = 1.0, jax.random.fold_in(rng, 6)
    for axis_at, parts in shards:
        steps = jnp.exp(jax.random.uniform(jax.random.fold_in(own, axis_at), (parts,), jnp.float32, least / len(shards), largest / len(shards)))
        loudness = loudness * jnp.repeat(steps, shape[axis_at] // parts).reshape([-1 if axis == axis_at else 1 for axis in range(len(shape))])
    return loudness


def noise(stream_key, dims, deviation, reach, split=(), kind=jnp.bfloat16):
    level = block_levels(stream_key, dims, split, -0.22, 0.18) if split else 1.0
    values = jax.random.normal(stream_key, dims, jnp.float32) * deviation * level
    return jnp.minimum(jnp.maximum(values, -reach), reach).astype(kind)


def setup_inputs(seed: int = 0) -> dict:
    streams_of = jax.random.split(jax.random.key(seed), 10)
    return {
        "latents": noise(streams_of[0], (TOKENS, LAT), 1.0, 6.0, ((0, 16),)),
        "sample_perturbation": noise(streams_of[1], (MEMBERS, TOKENS, LAT), 1.0, 6.0, ((0, 16), (1, 16))),
        "noise_table": jnp.clip(jax.random.uniform(streams_of[2], (TABLE, LAT), jnp.float32, 0.2, 1.5), 0.2, 1.5),
        "member_seed": touch_ends(jax.random.randint(streams_of[3], (MEMBERS,), 0, TABLE), jax.random.fold_in(streams_of[3], 1), 0, TABLE - 1).astype(jnp.int32),
        "piece_arrangement": jax.random.permutation(streams_of[4], REGION_ITEMS).astype(jnp.int32),
        "targets": noise(streams_of[5], (TOKENS, RESULT_DIM), 0.5, 4.0, ((0, 16),)),
        "w_gate": noise(streams_of[6], (LAT, HID), LAT ** -0.5, 0.25),
        "w_up": noise(streams_of[7], (LAT, HID), LAT ** -0.5, 0.25),
        "lowering_matrix": noise(streams_of[8], (HID, RESULT_DIM), HID ** -0.5, 0.1875),
    }


def apply_network(noisy_input, w_gate, w_up, lowering_matrix):
    sigmoid_branch_signal = jnp.dot(noisy_input, w_gate, preferred_element_type=jnp.float32)
    raising_signal = jnp.dot(noisy_input, w_up, preferred_element_type=jnp.float32)
    inner_signal = (sigmoid_branch_signal * jax.nn.sigmoid(sigmoid_branch_signal) * raising_signal).astype(jnp.bfloat16)
    predicted_values = jnp.dot(inner_signal, lowering_matrix, preferred_element_type=jnp.float32).astype(jnp.bfloat16)
    return (sigmoid_branch_signal, raising_signal, predicted_values)

def run_backward(cotangent, sigmoid_branch_signal, raising_signal, w_gate, w_up, lowering_matrix):
    hidden_grad = jnp.dot(cotangent, lowering_matrix.T, preferred_element_type=jnp.float32)
    sigmoid_gate = jax.nn.sigmoid(sigmoid_branch_signal)
    gate_grad = (hidden_grad * raising_signal * sigmoid_gate * (1.0 + sigmoid_branch_signal * (1.0 - sigmoid_gate))).astype(jnp.bfloat16)
    up_grad = (hidden_grad * sigmoid_branch_signal * sigmoid_gate).astype(jnp.bfloat16)
    first = jnp.dot(gate_grad, w_gate.T, preferred_element_type=jnp.float32)
    return first + jnp.dot(up_grad, w_up.T, preferred_element_type=jnp.float32)

def scoring_rule(predicted_item_matrix, observed_item_matrix):
    sample_discrepancy = predicted_item_matrix - observed_item_matrix
    return sample_discrepancy / jnp.sqrt(lax.optimization_barrier(jnp.sum(sample_discrepancy * sample_discrepancy, axis=-1, keepdims=True)) + 1.0)

def spread_fn(members_block, loss_scale):
    count = members_block.shape[0]
    wide_block = members_block.astype(jnp.float32)
    gram_matrix = jnp.einsum('mkf,nkf->kmn', wide_block, wide_block)
    diagonal = jnp.diagonal(gram_matrix, axis1=1, axis2=2)
    squared_gap = diagonal[:, :, None] + diagonal[:, None, :] - 2.0 * gram_matrix
    identity_mask = jnp.eye(count, dtype=bool)[None]
    distance = jnp.sqrt(jnp.where(identity_mask, 0.0, squared_gap) + 1.0)
    pair_weight = (1.0 / distance).astype(jnp.bfloat16)
    wide_weight = pair_weight.astype(jnp.float32)
    row_total = lax.optimization_barrier(jnp.sum(wide_weight, axis=2))
    weighted = jnp.einsum('kmn,nkf->mkf', wide_weight, wide_block)
    spread = loss_scale / count * (row_total.T[:, :, None] * wide_block - weighted)
    return spread.astype(jnp.bfloat16)

def reference(latents, sample_perturbation, noise_table, member_seed, piece_arrangement, targets, w_gate, w_up, lowering_matrix):
    sample_sequence = sample_perturbation.shape[0]
    region_blocks = latents.shape[0] // REGION_ITEMS
    embedding_matrix = PIECE_ITEMS * RESULT_DIM
    loss_scale = float(embedding_matrix) ** 0.5
    one_hot = (member_seed[:, None] == jnp.arange(TABLE, dtype=jnp.int32)[None, :]).astype(jnp.float32)
    component_multiplier = jnp.dot(one_hot, noise_table, precision=lax.Precision.HIGHEST)
    latent_rows = latents.astype(jnp.float32)

    def noisy(member_rows, member_scale):
        return (latent_rows + member_rows.astype(jnp.float32) * member_scale[None, :]).astype(jnp.bfloat16)

    def evaluate_ensemble_sample(paired):
        return apply_network(noisy(paired[0], paired[1]), w_gate, w_up, lowering_matrix)[2]
    predicted_values = lax.map(evaluate_ensemble_sample, (sample_perturbation, component_multiplier))
    piece_item_matrix = predicted_values.reshape(sample_sequence, region_blocks, REGION_ITEMS, RESULT_DIM)[:, :, piece_arrangement].reshape(sample_sequence, region_blocks * (REGION_ITEMS // PIECE_ITEMS), embedding_matrix)
    observed_item_matrix = targets.reshape(region_blocks, REGION_ITEMS, RESULT_DIM)[:, piece_arrangement].reshape(region_blocks * (REGION_ITEMS // PIECE_ITEMS), embedding_matrix).astype(jnp.float32)
    skill_term = scoring_rule(piece_item_matrix.astype(jnp.float32), observed_item_matrix[None])
    spread = spread_fn(piece_item_matrix, loss_scale)
    cotangent = (loss_scale * skill_term - spread.astype(jnp.float32)).astype(jnp.bfloat16)
    inverse_order = jnp.argsort(piece_arrangement).astype(jnp.int32)
    cotangent = cotangent.reshape(sample_sequence, region_blocks, REGION_ITEMS, RESULT_DIM)[:, :, inverse_order].reshape(sample_sequence, region_blocks * REGION_ITEMS, RESULT_DIM)

    def accumulate(total, triple):
        sigmoid_branch_signal, raising_signal, ignored = apply_network(noisy(triple[0], triple[1]), w_gate, w_up, lowering_matrix)
        return (total + run_backward(triple[2], sigmoid_branch_signal, raising_signal, w_gate, w_up, lowering_matrix), None)
    total, ignored = lax.scan(accumulate, jnp.zeros(latents.shape, jnp.float32), (sample_perturbation, component_multiplier, cotangent))
    return total
```

```python
import jax
import jax.numpy as jnp
from jax import lax
from jax.experimental import pallas as pl
from jax.experimental.pallas import tpu as pltpu
from jax.sharding import PartitionSpec as P

LAT = 512
HID = 1024
OUT = 384
PIECE = 8
GROUPS = 16
MINE = 48
LOCAL = 3
MEMBERS = 48
CHUNKS = (32, 16)
STARTS = (0, 32)
SCALE = float(PIECE * OUT) ** 0.5
F32 = jnp.float32
BF16 = jnp.bfloat16
VM = pl.BlockSpec(memory_space=pltpu.VMEM)
SM = pl.BlockSpec(memory_space=pltpu.SMEM)


def dot(a, b):
    return jnp.dot(a, b, preferred_element_type=F32)


def dot_t(a, b):
    return lax.dot_general(a, b, (((1,), (1,)), ((), ())), preferred_element_type=F32)


def pieces(x):
    high = x.astype(BF16)
    rest = x - high.astype(F32)
    mid = rest.astype(BF16)
    low = (rest - mid.astype(F32)).astype(BF16)
    return high, mid, low


def pack_kernel(me, seeds, order, latents, perturbation, table, targets, send0, send1, my_targets, pick):
    tokens = latents.shape[0]
    eye = lax.broadcasted_iota(jnp.int32, (128, 128), 0) == lax.broadcasted_iota(jnp.int32, (128, 128), 1)
    lane = lax.broadcasted_iota(jnp.int32, (128, tokens), 1)
    for b in range(tokens // 128):
        row = order[:, 128 * b : 128 * b + 128].astype(F32)
        column = jnp.sum(jnp.where(eye, row, 0.0), axis=1, keepdims=True).astype(jnp.int32)
        pick[128 * b : 128 * b + 128, :] = jnp.where(column == lane, 1.0, 0.0).astype(BF16)
    rows = latents[...].astype(F32)
    for m in range(LOCAL):
        factor = table[pl.ds(seeds[m], 1), :]
        noisy = (rows + perturbation[m].astype(F32) * factor).astype(BF16)
        moved = dot(pick[...], noisy).astype(BF16)
        for d in range(GROUPS):
            for send, start, count in zip((send0, send1), STARTS, CHUNKS):
                send[d, m * count : (m + 1) * count, :] = moved[d * MINE + start : d * MINE + start + count]
    mine = pick[pl.ds(pl.multiple_of(me[0] * MINE, 16), MINE), :]
    my_targets[...] = dot(mine, targets[...])


def score(forecast_ref, cotangent_ref, target, p, count):
    at = [pl.ds(p * PIECE + r, MEMBERS, stride=count) for r in range(PIECE)]
    u = jnp.concatenate([forecast_ref[j, a, :] for a in at for j in range(3)], axis=1)
    v = jnp.concatenate([target[p * PIECE + r : p * PIECE + r + 1, :] for r in range(PIECE)], axis=1)
    ub = u.astype(BF16)
    gram = dot_t(ub, ub)
    eye = lax.broadcasted_iota(jnp.int32, gram.shape, 0) == lax.broadcasted_iota(jnp.int32, gram.shape, 1)
    diagonal = jnp.where(eye, gram, 0.0)
    across = jnp.sum(diagonal, axis=1, keepdims=True)
    down = jnp.sum(diagonal, axis=0, keepdims=True)
    gap = across + down - 2.0 * gram
    weight = (1.0 / jnp.sqrt(jnp.where(eye, 0.0, gap) + 1.0)).astype(BF16)
    total = jnp.sum(weight.astype(F32), axis=1, keepdims=True)
    spread = (SCALE / MEMBERS * (total * u - dot(weight, ub))).astype(BF16)
    miss = u - v
    norm = jnp.sum(miss * miss, axis=1, keepdims=True)
    skill = miss * (1.0 / jnp.sqrt(norm + 1.0))
    cotangent = SCALE * skill - spread.astype(F32)
    for r, a in enumerate(at):
        for j in range(3):
            cotangent_ref[j, a, :] = cotangent[:, OUT * r + 128 * j : OUT * r + 128 * j + 128]


def network(noisy, target, w_gate, w_up, lowering, left, right, forecast, cotangent, count):
    total = MEMBERS * count
    block = 256

    @pl.loop(0, total // block)
    def _(i):
        at = pl.ds(pl.multiple_of(i * block, block), block)
        x = noisy[at, :]
        gate = dot(x, w_gate[...])
        up = dot(x, w_up[...])
        s = jax.nn.sigmoid(gate)
        swish = gate * s
        right[at, :] = swish
        left[at, :] = up * (s + swish * (1.0 - s))
        made = dot((swish * up).astype(BF16), lowering[...]).astype(BF16).astype(F32)
        for j in range(3):
            forecast[j, at, :] = made[:, 128 * j : 128 * j + 128]

    for p in range(count // PIECE):
        score(forecast, cotangent, target, p, count)

    token = lax.broadcasted_iota(jnp.int32, (count, block), 0)
    place = lax.broadcasted_iota(jnp.int32, (count, block), 1)
    gate_sum = jnp.zeros((count, HID), F32)
    up_sum = jnp.zeros((count, HID), F32)

    def step(i, carry):
        gate_sum, up_sum = carry
        at = pl.ds(pl.multiple_of(i * block, block), block)
        hidden_grad = dot_t(
            jnp.concatenate([cotangent[j, at, :] for j in range(3)], axis=1).astype(BF16), lowering[...]
        )
        gate_grad = (hidden_grad * left[at, :]).astype(BF16)
        up_grad = (hidden_grad * right[at, :]).astype(BF16)
        collect = jnp.where(lax.rem(place, count) == token, 1.0, 0.0).astype(BF16)
        return gate_sum + dot(collect, gate_grad), up_sum + dot(collect, up_grad)

    gate_sum, up_sum = lax.fori_loop(0, total // block, step, (gate_sum, up_sum))
    gates = dot_t(jnp.concatenate(pieces(gate_sum), axis=0), w_gate[...])
    ups = dot_t(jnp.concatenate(pieces(up_sum), axis=0), w_up[...])
    both = gates + ups
    return both[:count] + both[count : 2 * count] + both[2 * count :]


def first_kernel(noisy, target, w_gate, w_up, lowering, out, left, right, forecast, cotangent):
    grad = network(noisy, target[: CHUNKS[0]], w_gate, w_up, lowering, left, right, forecast, cotangent, CHUNKS[0])
    out[...] = grad


def last_kernel(noisy, target, w_gate, w_up, lowering, earlier, out, left, right, forecast, cotangent):
    grad = network(noisy, target[CHUNKS[0] :], w_gate, w_up, lowering, left, right, forecast, cotangent, CHUNKS[1])
    parts = (earlier[:16], earlier[16:], grad)
    blank = jnp.zeros((16, 32), F32)
    for d in range(GROUPS):
        out[d] = jnp.concatenate([part[:, 32 * d : 32 * d + 32] for part in parts] + [blank], axis=1)


def unpack_kernel(arrived, pick, out):
    flat = arrived[...].reshape(GROUPS * 16, 128)
    turned = flat.T
    total = jnp.zeros(out.shape, F32)
    for c in range(3):
        rows = jnp.concatenate([pick[d * MINE + 16 * c : d * MINE + 16 * c + 16, :] for d in range(GROUPS)], axis=0)
        placed = dot(jnp.concatenate(pieces(turned[32 * c : 32 * c + 32]), axis=0), rows)
        total = total + placed[:32] + placed[32:64] + placed[64:]
    out[...] = total


def call(kernel, out_shape, specs, scratch=(), flops=0):
    many = isinstance(out_shape, list)
    return pl.pallas_call(
        kernel,
        out_shape=out_shape,
        in_specs=specs,
        out_specs=[VM] * len(out_shape) if many else VM,
        scratch_shapes=list(scratch),
        compiler_params=pltpu.CompilerParams(vmem_limit_bytes=48 * 1024 * 1024),
        cost_estimate=pl.CostEstimate(flops=flops, transcendentals=0, bytes_accessed=0) if flops else None,
    )


def scratch(count):
    rows = MEMBERS * count
    return (
        pltpu.VMEM((rows, HID), F32),
        pltpu.VMEM((rows, HID), F32),
        pltpu.VMEM((3, rows, 128), F32),
        pltpu.VMEM((3, rows, 128), F32),
    )


def body(latents, perturbation, noise_table, member_seed, piece_arrangement, targets, w_gate, w_up, lowering_matrix):
    tokens = latents.shape[0]
    me = lax.axis_index("member").astype(jnp.int32).reshape(1)
    shape = jax.ShapeDtypeStruct
    sends = [shape((GROUPS, LOCAL * count, LAT), BF16) for count in CHUNKS]
    send0, send1, my_targets, pick = call(
        pack_kernel,
        [*sends, shape((MINE, OUT), F32), shape((tokens, tokens), BF16)],
        [SM, SM, VM, VM, VM, VM, VM],
    )(me, member_seed, piece_arrangement.reshape(1, tokens), latents, perturbation, noise_table, targets)
    got0 = lax.all_to_all(send0, "member", 0, 0, tiled=True)
    got1 = lax.all_to_all(send1, "member", 0, 0, tiled=True)
    earlier = call(first_kernel, shape((CHUNKS[0], LAT), F32), [VM] * 5, scratch(CHUNKS[0]), 10**10)(
        got0.reshape(MEMBERS * CHUNKS[0], LAT), my_targets, w_gate, w_up, lowering_matrix
    )
    packed = call(last_kernel, shape((GROUPS, 16, 128), F32), [VM] * 6, scratch(CHUNKS[1]), 5 * 10**9)(
        got1.reshape(MEMBERS * CHUNKS[1], LAT), my_targets, w_gate, w_up, lowering_matrix, earlier
    )
    arrived = lax.all_to_all(packed, "member", 0, 0, tiled=True)
    columns = call(unpack_kernel, shape((LAT // GROUPS, tokens), F32), [VM] * 2)(arrived, pick)
    return columns.T


def solution(mesh):
    in_specs = (
        P("space", None),
        P("member", "space", None),
        P(),
        P("member"),
        P(),
        P("space", None),
        P(),
        P(),
        P(),
    )
    return jax.shard_map(body, mesh=mesh, in_specs=in_specs, out_specs=P("space", "member"), check_vma=False)
```

```python
import jax
import jax.numpy as jnp
from jax import lax
from jax.experimental import pallas as pl
from jax.experimental.pallas import tpu as pltpu
from jax.sharding import PartitionSpec as P


LAT = 512
HID = 1024
OUT = 384
PIECE = 8
BLOCK = 256
PAD = 8
GROUPS = 16
MINE = 48
LOCAL = 3
MEMBERS = 48
Z = 8
OFFSETS = tuple((dz, dc) for dz in (0, 3, 5, 4, 2, 6, 1, 7) for dc in (0, 1))
CHUNKS = (32, 16)
STARTS = (0, 32)
SCALE = float(PIECE * OUT) ** 0.5
F32 = jnp.float32
BF16 = jnp.bfloat16
VM = pl.BlockSpec(memory_space=pltpu.VMEM)
SM = pl.BlockSpec(memory_space=pltpu.SMEM)
HB = pl.BlockSpec(memory_space=pltpu.HBM)


def far(x):
    return pltpu.with_memory_space_constraint(x, pltpu.HBM)


def dot(a, b):
    return jnp.dot(a, b, preferred_element_type=F32)


def dot_t(a, b):
    return lax.dot_general(a, b, (((1,), (1,)), ((), ())), preferred_element_type=F32)


def pieces(x):
    high = x.astype(BF16)
    rest = x - high.astype(F32)
    mid = rest.astype(BF16)
    low = (rest - mid.astype(F32)).astype(BF16)
    return high, mid, low


def columns_of(order):
    eye = lax.broadcasted_iota(jnp.int32, (128, 128), 0) == lax.broadcasted_iota(jnp.int32, (128, 128), 1)
    found = []
    for b in range(order.shape[1] // 128):
        row = order[:, 128 * b : 128 * b + 128].astype(F32)
        found.append(jnp.sum(jnp.where(eye, row, 0.0), axis=1, keepdims=True).astype(jnp.int32))
    return found


def one_hot(columns, start, count, tokens):
    lane = lax.broadcasted_iota(jnp.int32, (16, tokens), 1)
    parts = []
    for d in range(GROUPS):
        for first in range(d * MINE + start, d * MINE + start + count, 16):
            column = columns[first // 128][first % 128 : first % 128 + 16]
            parts.append(jnp.where(column == lane, 1.0, 0.0).astype(BF16))
    return jnp.concatenate(parts, axis=0)


def move(noisy, picked, send, count):
    for m in range(LOCAL):
        moved = dot(picked, noisy(m)).astype(BF16)
        for d in range(GROUPS):
            send[d, m * count : (m + 1) * count, :] = moved[d * count : (d + 1) * count]


def load_state(seeds, latents, perturbation, table, seeds_here, latents_here, here, table_here, sems):
    copies = [
        pltpu.make_async_copy(seeds, seeds_here, sems.at[0]),
        pltpu.make_async_copy(table, table_here, sems.at[1]),
        pltpu.make_async_copy(latents, latents_here, sems.at[2]),
    ] + [pltpu.make_async_copy(perturbation.at[m], here.at[m], sems.at[3 + m]) for m in range(LOCAL)]
    for copy in copies:
        copy.start()

    def noisy(m):
        if m == 0:
            for copy in copies[:3]:
                copy.wait()
        copies[3 + m].wait()
        factor = table_here[pl.ds(seeds_here[m], 1), :]
        return (latents_here[...].astype(F32) + here[m].astype(F32) * factor).astype(BF16)

    return noisy


def early_kernel(order, seeds, latents, perturbation, table, send, *state):
    noisy = load_state(seeds, latents, perturbation, table, *state)
    picked = one_hot(columns_of(order[...]), STARTS[0], CHUNKS[0], latents.shape[0])
    move(noisy, picked, send, CHUNKS[0])


def late_kernel(me, order, seeds, latents, perturbation, table, *rest):
    sends, pick, state = rest[:GROUPS], rest[GROUPS], rest[GROUPS + 1 :]
    noisy = load_state(seeds, latents, perturbation, table, *state)
    pick[...] = one_hot(columns_of(order[...]), 0, MINE, latents.shape[0])
    z, core = me[0] // 2, lax.rem(me[0], 2)
    count = CHUNKS[1]
    parts = []
    for dz, dc in OFFSETS:
        there = lax.rem(z + dz, Z) * 2 + (1 - core if dc else core)
        parts.append(pick[pl.ds(pl.multiple_of(there * MINE + STARTS[1], 16), count), :])
    picked = jnp.concatenate(parts, axis=0)
    for m in range(LOCAL):
        moved = dot(picked, noisy(m)).astype(BF16)
        for k, send in enumerate(sends):
            send[m * count : (m + 1) * count, :] = moved[k * count : (k + 1) * count]


def target_kernel(me, pick, targets, my_targets):
    my_targets[...] = dot(pick[pl.ds(pl.multiple_of(me[0] * MINE, 16), MINE), :], targets[...])


def score(forecast, cotangent, target, p, gap_rows):
    def token(r):
        at = pl.ds(p * PIECE + r, MEMBERS, stride=gap_rows)
        u = jnp.concatenate([forecast[j, at, :] for j in range(3)], axis=1)
        return at, u, u - target[p * PIECE + r : p * PIECE + r + 1, :]

    gram = jnp.zeros((MEMBERS, MEMBERS), F32)
    norm = jnp.zeros((MEMBERS, 128), F32)
    for r in range(PIECE):
        at, u, miss = token(r)
        ub = u.astype(BF16)
        gram = gram + dot_t(ub, ub)
        square = miss * miss
        norm = norm + square[:, :128] + square[:, 128:256] + square[:, 256:]
    eye = lax.broadcasted_iota(jnp.int32, gram.shape, 0) == lax.broadcasted_iota(jnp.int32, gram.shape, 1)
    diagonal = jnp.where(eye, gram, 0.0)
    across = jnp.sum(diagonal, axis=1, keepdims=True)
    down = jnp.sum(diagonal, axis=0, keepdims=True)
    gap = across + down - 2.0 * gram
    weight = (1.0 / jnp.sqrt(jnp.where(eye, 0.0, gap) + 1.0)).astype(BF16)
    total = jnp.sum(weight.astype(F32), axis=1, keepdims=True)
    skill = SCALE / jnp.sqrt(jnp.sum(norm, axis=1, keepdims=True) + 1.0)
    for r in range(PIECE):
        at, u, miss = token(r)
        spread = (SCALE / MEMBERS * (total * u - dot(weight, u.astype(BF16)))).astype(BF16)
        made = skill * miss - spread.astype(F32)
        for j in range(3):
            cotangent[j, at, :] = made[:, 128 * j : 128 * j + 128]


def network(noisy, target, w_gate, w_up, lowering, state, count, start):
    left, right, forecast, cotangent, gate_sum, up_sum, target_here, sem = state[:8]
    copy = pltpu.make_async_copy(target.at[pl.ds(start, count)], target_here, sem)
    copy.start()
    total = MEMBERS * count
    block = BLOCK
    inside = block // count
    gap_rows = count + PAD

    @pl.loop(0, total // block)
    def _(i):
        at = pl.ds(pl.multiple_of(i * block, block), block)
        x = noisy[at, :]
        half = 0.5 * dot(x, w_gate[...])
        up = dot(x, w_up[...])
        bent = 1.0 + jnp.tanh(half)
        swish = half * bent
        s = 0.5 * bent
        right[at, :] = swish
        left[at, :] = up * (s + swish * (1.0 - s))
        made = dot((swish * up).astype(BF16), lowering[...]).astype(BF16).astype(F32)
        for q in range(inside):
            to = pl.ds(pl.multiple_of(i * inside * gap_rows + q * gap_rows, 8), count)
            for j in range(3):
                forecast[j, to, :] = made[count * q : count * q + count, 128 * j : 128 * j + 128]

    copy.wait()
    for p in range(count // PIECE):
        score(forecast, cotangent, target_here, p, gap_rows)

    token = lax.broadcasted_iota(jnp.int32, (count, block), 0)
    place = lax.broadcasted_iota(jnp.int32, (count, block), 1)
    collect = jnp.where(lax.rem(place, count) == token, 1.0, 0.0).astype(BF16)
    gate_sum[...] = jnp.zeros((count, HID), F32)
    up_sum[...] = jnp.zeros((count, HID), F32)

    @pl.loop(0, total // block)
    def _(i):
        at = pl.ds(pl.multiple_of(i * block, block), block)
        rows = []
        for q in range(inside):
            back = pl.ds(pl.multiple_of(i * inside * gap_rows + q * gap_rows, 8), count)
            rows.append(jnp.concatenate([cotangent[j, back, :] for j in range(3)], axis=1))
        hidden_grad = dot_t(jnp.concatenate(rows, axis=0).astype(BF16), lowering[...])
        gate_sum[...] += dot(collect, (hidden_grad * left[at, :]).astype(BF16))
        up_sum[...] += dot(collect, (hidden_grad * right[at, :]).astype(BF16))

    gates = dot_t(jnp.concatenate(pieces(gate_sum[...]), axis=0), w_gate[...])
    ups = dot_t(jnp.concatenate(pieces(up_sum[...]), axis=0), w_up[...])
    both = gates + ups
    return both[:count] + both[count : 2 * count] + both[2 * count :]


def first_kernel(noisy, target, w_gate, w_up, lowering, out, gate_here, up_here, low_here, *state):
    here, sem, sems = state[-3:]
    copies = [
        pltpu.make_async_copy(w_gate, gate_here, sems.at[0]),
        pltpu.make_async_copy(w_up, up_here, sems.at[1]),
        pltpu.make_async_copy(lowering, low_here, sems.at[2]),
    ]
    for copy in copies:
        copy.start()
    for copy in copies:
        copy.wait()
    here[...] = network(noisy, target, gate_here, up_here, low_here, state, CHUNKS[0], STARTS[0])
    copy = pltpu.make_async_copy(here, out, sem)
    copy.start()
    copy.wait()


def last_kernel(*refs):
    gathered, (target, w_gate, w_up, lowering, earlier, out), state = refs[:GROUPS], refs[GROUPS : GROUPS + 6], refs[GROUPS + 6 :]
    here, sem, noisy = state[-3:]
    copy = pltpu.make_async_copy(earlier, here, sem)
    copy.start()
    size = LOCAL * CHUNKS[1]
    for k, part in enumerate(gathered):
        noisy[k * size : (k + 1) * size, :] = part[...]
    grad = network(noisy, target, w_gate, w_up, lowering, state, CHUNKS[1], STARTS[1])
    copy.wait()
    parts = (here[:16], here[16:], grad)
    blank = jnp.zeros((16, 32), F32)
    for d in range(GROUPS):
        out[d] = jnp.concatenate([part[:, 32 * d : 32 * d + 32] for part in parts] + [blank], axis=1)


def unpack_kernel(arrived, pick, out):
    flat = arrived[...].reshape(GROUPS * 16, 128)
    turned = flat.T
    total = jnp.zeros(out.shape, F32)
    for c in range(3):
        rows = jnp.concatenate([pick[d * MINE + 16 * c : d * MINE + 16 * c + 16, :] for d in range(GROUPS)], axis=0)
        placed = dot(jnp.concatenate(pieces(turned[32 * c : 32 * c + 32]), axis=0), rows)
        total = total + placed[:32] + placed[32:64] + placed[64:]
    out[...] = total


def call(kernel, out_shape, specs, out_specs, scratch=(), flops=0, megabytes=24):
    return pl.pallas_call(
        kernel,
        out_shape=out_shape,
        in_specs=specs,
        out_specs=out_specs,
        scratch_shapes=list(scratch),
        compiler_params=pltpu.CompilerParams(vmem_limit_bytes=megabytes * 1024 * 1024),
        cost_estimate=pl.CostEstimate(flops=flops, transcendentals=0, bytes_accessed=0) if flops else None,
    )


def scratch(count):
    rows = MEMBERS * count
    padded = MEMBERS * (count + PAD)
    return (
        pltpu.VMEM((rows, HID), F32),
        pltpu.VMEM((rows, HID), F32),
        pltpu.VMEM((3, padded, 128), F32),
        pltpu.VMEM((3, padded, 128), F32),
        pltpu.VMEM((count, HID), F32),
        pltpu.VMEM((count, HID), F32),
        pltpu.VMEM((count, OUT), F32),
        pltpu.SemaphoreType.DMA,
        pltpu.VMEM((CHUNKS[0], LAT), F32),
        pltpu.SemaphoreType.DMA,
    )


def body(latents, perturbation, noise_table, member_seed, piece_arrangement, targets, w_gate, w_up, lowering_matrix):
    tokens = latents.shape[0]
    latents, perturbation, noise_table, member_seed, targets = (
        far(x) for x in (latents, perturbation, noise_table, member_seed, targets)
    )
    me = lax.axis_index("member").astype(jnp.int32).reshape(1)
    shape = jax.ShapeDtypeStruct
    order = piece_arrangement.reshape(1, tokens)
    state = (
        pltpu.SMEM((LOCAL,), jnp.int32),
        pltpu.VMEM((tokens, LAT), BF16),
        pltpu.VMEM((LOCAL, tokens, LAT), BF16),
        pltpu.VMEM(noise_table.shape, F32),
        pltpu.SemaphoreType.DMA((3 + LOCAL,)),
    )
    send0 = call(early_kernel, shape((GROUPS, LOCAL * CHUNKS[0], LAT), BF16), [VM] + [HB] * 4, VM, state, megabytes=20)(
        order, member_seed, latents, perturbation, noise_table
    )
    got0 = lax.all_to_all(send0, "member", 0, 0, tiled=True)
    *sends, pick = call(
        late_kernel,
        [shape((LOCAL * CHUNKS[1], LAT), BF16)] * GROUPS + [shape((tokens, tokens), BF16)],
        [SM, VM] + [HB] * 4,
        [VM] * (GROUPS + 1),
        state,
        flops=10**9,
        megabytes=20,
    )(me, order, member_seed, latents, perturbation, noise_table)
    got1 = []
    for (dz, dc), send in zip(OFFSETS, sends):
        pairs = [(2 * z + c, (z + dz) % Z * 2 + (c ^ dc)) for z in range(Z) for c in range(2)]
        got1.append(send if dz == dc == 0 else lax.ppermute(send, "member", pairs))
    my_targets = call(target_kernel, pltpu.HBM((MINE, OUT), F32), [SM, VM, VM], VM, flops=10**7, megabytes=4)(
        me, pick, targets
    )
    my_targets = far(my_targets)
    weights = tuple(far(w) for w in (w_gate, w_up, lowering_matrix))
    earlier, *weights = call(
        first_kernel,
        [pltpu.HBM((CHUNKS[0], LAT), F32), *(shape(w.shape, BF16) for w in weights)],
        [VM] + [HB] * 4,
        [HB] + [VM] * 3,
        (*scratch(CHUNKS[0]), pltpu.SemaphoreType.DMA((3,))),
        10**10,
        32,
    )(got0.reshape(MEMBERS * CHUNKS[0], LAT), my_targets, *weights)
    extra = (*scratch(CHUNKS[1]), pltpu.VMEM((MEMBERS * CHUNKS[1], LAT), BF16))
    packed = call(
        last_kernel, shape((GROUPS, 16, 128), F32), [VM] * GROUPS + [HB, VM, VM, VM, HB], VM, extra, 5 * 10**9, 24
    )(*got1, my_targets, *weights, far(earlier))
    arrived = lax.all_to_all(packed, "member", 0, 0, tiled=True)
    columns = call(unpack_kernel, shape((LAT // GROUPS, tokens), F32), [VM] * 2, VM)(arrived, pick)
    return columns.T


def solution(mesh):
    in_specs = (
        P("space", None),
        P("member", "space", None),
        P(),
        P("member"),
        P(),
        P("space", None),
        P(),
        P(),
        P(),
    )
    return jax.shard_map(body, mesh=mesh, in_specs=in_specs, out_specs=P("space", "member"), check_vma=False)
```

```python
import jax
import jax.numpy as jnp
from jax import lax
from jax.experimental import pallas as pl
from jax.experimental.pallas import tpu as pltpu
from jax.sharding import PartitionSpec as P


LAT = 512
HID = 1024
OUT = 384
PIECE = 8
BLOCK = 256
PAD = 8
GROUPS = 16
MINE = 48
LOCAL = 3
MEMBERS = 48
Z = 8
OFFSETS = tuple((dz, dc) for dz in (1, 7, 3, 5, 4, 2, 6, 0) for dc in (0, 1))
CHUNKS = (32, 16)
STARTS = (0, 32)
SCALE = float(PIECE * OUT) ** 0.5
F32 = jnp.float32
BF16 = jnp.bfloat16
VM = pl.BlockSpec(memory_space=pltpu.VMEM)
SM = pl.BlockSpec(memory_space=pltpu.SMEM)
HB = pl.BlockSpec(memory_space=pltpu.HBM)


def far(x):
    return pltpu.with_memory_space_constraint(x, pltpu.HBM)


def dot(a, b):
    return jnp.dot(a, b, preferred_element_type=F32)


def dot_t(a, b):
    return lax.dot_general(a, b, (((1,), (1,)), ((), ())), preferred_element_type=F32)


def pieces(x):
    high = x.astype(BF16)
    rest = x - high.astype(F32)
    mid = rest.astype(BF16)
    low = (rest - mid.astype(F32)).astype(BF16)
    return high, mid, low


def columns_of(order):
    eye = lax.broadcasted_iota(jnp.int32, (128, 128), 0) == lax.broadcasted_iota(jnp.int32, (128, 128), 1)
    found = []
    for b in range(order.shape[0] // 128):
        row = order[pl.ds(128 * b, 128)].reshape(1, 128).astype(F32)
        found.append(jnp.sum(jnp.where(eye, row, 0.0), axis=1, keepdims=True).astype(jnp.int32))
    return found


def one_hot(columns, start, count, tokens):
    lane = lax.broadcasted_iota(jnp.int32, (16, tokens), 1)
    parts = []
    for d in range(GROUPS):
        for first in range(d * MINE + start, d * MINE + start + count, 16):
            column = columns[first // 128][first % 128 : first % 128 + 16]
            parts.append(jnp.where(column == lane, 1.0, 0.0).astype(BF16))
    return jnp.concatenate(parts, axis=0)


def move(noisy, picked, send, count):
    for m in range(LOCAL):
        moved = dot(picked, noisy(m)).astype(BF16)
        for d in range(GROUPS):
            send[d, m * count : (m + 1) * count, :] = moved[d * count : (d + 1) * count]


def load_state(order, seeds, latents, perturbation, table, order_here, seeds_here, latents_here, here, table_here, sems):
    first = pltpu.make_async_copy(order, order_here, sems.at[3 + LOCAL])
    first.start()
    copies = [
        pltpu.make_async_copy(seeds, seeds_here, sems.at[0]),
        pltpu.make_async_copy(table, table_here, sems.at[1]),
        pltpu.make_async_copy(latents, latents_here, sems.at[2]),
    ] + [pltpu.make_async_copy(perturbation.at[m], here.at[m], sems.at[3 + m]) for m in range(LOCAL)]
    for copy in copies:
        copy.start()
    first.wait()

    def noisy(m):
        if m == 0:
            for copy in copies[:3]:
                copy.wait()
        copies[3 + m].wait()
        factor = table_here[pl.ds(seeds_here[m], 1), :]
        return (latents_here[...].astype(F32) + here[m].astype(F32) * factor).astype(BF16)

    return noisy


def early_kernel(me, order, seeds, latents, perturbation, table, *rest):
    sends, state, pick = rest[:GROUPS], rest[GROUPS:-1], rest[-1]
    noisy = load_state(order, seeds, latents, perturbation, table, *state)
    count = CHUNKS[0]
    pick[...] = one_hot(columns_of(state[0]), STARTS[0], count, latents.shape[0])
    z, core = me[0] // 2, lax.rem(me[0], 2)
    parts = []
    for dz, dc in OFFSETS:
        there = lax.rem(z + dz, Z) * 2 + (1 - core if dc else core)
        parts.append(pick[pl.ds(pl.multiple_of(there * count, 16), count), :])
    picked = jnp.concatenate(parts, axis=0)
    for m in range(LOCAL):
        moved = dot(picked, noisy(m)).astype(BF16)
        for k, send in enumerate(sends):
            send[m * count : (m + 1) * count, :] = moved[k * count : (k + 1) * count]


def late_kernel(order, seeds, latents, perturbation, table, send, pick, *state):
    noisy = load_state(order, seeds, latents, perturbation, table, *state)
    columns = columns_of(state[0])
    pick[...] = one_hot(columns, 0, MINE, latents.shape[0])
    move(noisy, one_hot(columns, STARTS[1], CHUNKS[1], latents.shape[0]), send, CHUNKS[1])


def target_kernel(me, pick, targets, w_gate, w_up, lowering, my_targets, gate_here, up_here, low_here):
    my_targets[...] = dot(pick[pl.ds(pl.multiple_of(me[0] * MINE, 16), MINE), :], targets[...])
    gate_here[...] = w_gate[...]
    up_here[...] = w_up[...]
    low_here[...] = lowering[...]


def score(forecast, cotangent, target, p, gap_rows):
    def token(r):
        at = pl.ds(p * PIECE + r, MEMBERS, stride=gap_rows)
        u = jnp.concatenate([forecast[j, at, :] for j in range(3)], axis=1)
        return at, u, u - target[p * PIECE + r : p * PIECE + r + 1, :]

    gram = jnp.zeros((MEMBERS, MEMBERS), F32)
    norm = jnp.zeros((MEMBERS, 128), F32)
    for r in range(PIECE):
        at, u, miss = token(r)
        ub = u.astype(BF16)
        gram = gram + dot_t(ub, ub)
        square = miss * miss
        norm = norm + square[:, :128] + square[:, 128:256] + square[:, 256:]
    eye = lax.broadcasted_iota(jnp.int32, gram.shape, 0) == lax.broadcasted_iota(jnp.int32, gram.shape, 1)
    diagonal = jnp.where(eye, gram, 0.0)
    across = jnp.sum(diagonal, axis=1, keepdims=True)
    down = jnp.sum(diagonal, axis=0, keepdims=True)
    gap = across + down - 2.0 * gram
    weight = (1.0 / jnp.sqrt(jnp.where(eye, 0.0, gap) + 1.0)).astype(BF16)
    total = jnp.sum(weight.astype(F32), axis=1, keepdims=True)
    skill = SCALE / jnp.sqrt(jnp.sum(norm, axis=1, keepdims=True) + 1.0)
    for r in range(PIECE):
        at, u, miss = token(r)
        spread = (SCALE / MEMBERS * (total * u - dot(weight, u.astype(BF16)))).astype(BF16)
        made = skill * miss - spread.astype(F32)
        for j in range(3):
            cotangent[j, at, :] = made[:, 128 * j : 128 * j + 128]


def network(noisy, target, w_gate, w_up, lowering, state, count, start):
    left, right, forecast, cotangent, gate_sum, up_sum, target_here, sem = state[:8]
    copy = pltpu.make_async_copy(target.at[pl.ds(start, count)], target_here, sem)
    copy.start()
    total = MEMBERS * count
    block = BLOCK
    inside = block // count
    gap_rows = count + PAD

    @pl.loop(0, total // block)
    def _(i):
        at = pl.ds(pl.multiple_of(i * block, block), block)
        x = noisy[at, :]
        half = 0.5 * dot(x, w_gate[...])
        up = dot(x, w_up[...])
        bent = 1.0 + jnp.tanh(half)
        swish = half * bent
        s = 0.5 * bent
        right[at, :] = swish
        left[at, :] = up * (s + swish * (1.0 - s))
        made = dot((swish * up).astype(BF16), lowering[...]).astype(BF16).astype(F32)
        for q in range(inside):
            to = pl.ds(pl.multiple_of(i * inside * gap_rows + q * gap_rows, 8), count)
            for j in range(3):
                forecast[j, to, :] = made[count * q : count * q + count, 128 * j : 128 * j + 128]

    copy.wait()
    for p in range(count // PIECE):
        score(forecast, cotangent, target_here, p, gap_rows)

    token = lax.broadcasted_iota(jnp.int32, (count, block), 0)
    place = lax.broadcasted_iota(jnp.int32, (count, block), 1)
    collect = jnp.where(lax.rem(place, count) == token, 1.0, 0.0).astype(BF16)
    gate_sum[...] = jnp.zeros((count, HID), F32)
    up_sum[...] = jnp.zeros((count, HID), F32)

    @pl.loop(0, total // block)
    def _(i):
        at = pl.ds(pl.multiple_of(i * block, block), block)
        rows = []
        for q in range(inside):
            back = pl.ds(pl.multiple_of(i * inside * gap_rows + q * gap_rows, 8), count)
            rows.append(jnp.concatenate([cotangent[j, back, :] for j in range(3)], axis=1))
        hidden_grad = dot_t(jnp.concatenate(rows, axis=0).astype(BF16), lowering[...])
        gate_sum[...] += dot(collect, (hidden_grad * left[at, :]).astype(BF16))
        up_sum[...] += dot(collect, (hidden_grad * right[at, :]).astype(BF16))

    gates = dot_t(jnp.concatenate(pieces(gate_sum[...]), axis=0), w_gate[...])
    ups = dot_t(jnp.concatenate(pieces(up_sum[...]), axis=0), w_up[...])
    both = gates + ups
    return both[:count] + both[count : 2 * count] + both[2 * count :]


def first_kernel(*refs):
    gathered, (target, w_gate, w_up, lowering, out), state = refs[:GROUPS], refs[GROUPS : GROUPS + 5], refs[GROUPS + 5 :]
    here, sem, noisy, sems = state[-4:]
    size = LOCAL * CHUNKS[0]
    copies = [
        pltpu.make_async_copy(part, noisy.at[pl.ds(k * size, size)], sems.at[k]) for k, part in enumerate(gathered)
    ]
    for copy in copies:
        copy.start()
    for copy in copies:
        copy.wait()
    here[...] = network(noisy, target, w_gate, w_up, lowering, state, CHUNKS[0], STARTS[0])
    copy = pltpu.make_async_copy(here, out, sem)
    copy.start()
    copy.wait()


def last_kernel(noisy, target, w_gate, w_up, lowering, earlier, out, *state):
    here, sem, gate_here, up_here, low_here, sems = state[-6:]
    copies = [
        pltpu.make_async_copy(w_gate, gate_here, sems.at[0]),
        pltpu.make_async_copy(w_up, up_here, sems.at[1]),
        pltpu.make_async_copy(lowering, low_here, sems.at[2]),
        pltpu.make_async_copy(earlier, here, sem),
    ]
    for copy in copies:
        copy.start()
    for copy in copies:
        copy.wait()
    grad = network(noisy, target, gate_here, up_here, low_here, state, CHUNKS[1], STARTS[1])
    parts = (here[:16], here[16:], grad)
    blank = jnp.zeros((16, 32), F32)
    for d in range(GROUPS):
        out[d] = jnp.concatenate([part[:, 32 * d : 32 * d + 32] for part in parts] + [blank], axis=1)


def unpack_kernel(arrived, pick, out):
    flat = arrived[...].reshape(GROUPS * 16, 128)
    turned = flat.T
    total = jnp.zeros(out.shape, F32)
    for c in range(3):
        rows = jnp.concatenate([pick[d * MINE + 16 * c : d * MINE + 16 * c + 16, :] for d in range(GROUPS)], axis=0)
        placed = dot(jnp.concatenate(pieces(turned[32 * c : 32 * c + 32]), axis=0), rows)
        total = total + placed[:32] + placed[32:64] + placed[64:]
    out[...] = total


def call(kernel, out_shape, specs, out_specs, scratch=(), flops=0, megabytes=24):
    return pl.pallas_call(
        kernel,
        out_shape=out_shape,
        in_specs=specs,
        out_specs=out_specs,
        scratch_shapes=list(scratch),
        compiler_params=pltpu.CompilerParams(vmem_limit_bytes=megabytes * 1024 * 1024),
        cost_estimate=pl.CostEstimate(flops=flops, transcendentals=0, bytes_accessed=0) if flops else None,
    )


def scratch(count):
    rows = MEMBERS * count
    padded = MEMBERS * (count + PAD)
    return (
        pltpu.VMEM((rows, HID), F32),
        pltpu.VMEM((rows, HID), F32),
        pltpu.VMEM((3, padded, 128), F32),
        pltpu.VMEM((3, padded, 128), F32),
        pltpu.VMEM((count, HID), F32),
        pltpu.VMEM((count, HID), F32),
        pltpu.VMEM((count, OUT), F32),
        pltpu.SemaphoreType.DMA,
        pltpu.VMEM((CHUNKS[0], LAT), F32),
        pltpu.SemaphoreType.DMA,
    )


def body(latents, perturbation, noise_table, member_seed, piece_arrangement, targets, w_gate, w_up, lowering_matrix):
    tokens = latents.shape[0]
    latents, perturbation, noise_table, member_seed, targets = (
        far(x) for x in (latents, perturbation, noise_table, member_seed, targets)
    )
    me = lax.axis_index("member").astype(jnp.int32).reshape(1)
    shape = jax.ShapeDtypeStruct
    order = far(piece_arrangement)
    state = (
        pltpu.VMEM((tokens,), jnp.int32),
        pltpu.SMEM((LOCAL,), jnp.int32),
        pltpu.VMEM((tokens, LAT), BF16),
        pltpu.VMEM((LOCAL, tokens, LAT), BF16),
        pltpu.VMEM(noise_table.shape, F32),
        pltpu.SemaphoreType.DMA((4 + LOCAL,)),
    )
    sends = call(
        early_kernel,
        [(shape if any(o) else pltpu.HBM)((LOCAL * CHUNKS[0], LAT), BF16) for o in OFFSETS],
        [SM] + [HB] * 5,
        [VM] * GROUPS,
        (*state, pltpu.VMEM((GROUPS * CHUNKS[0], tokens), BF16)),
        megabytes=16,
    )(me, order, member_seed, latents, perturbation, noise_table)
    got0 = []
    for (dz, dc), send in zip(OFFSETS, sends):
        pairs = [(2 * z + c, (z + dz) % Z * 2 + (c ^ dc)) for z in range(Z) for c in range(2)]
        got0.append(send if dz == dc == 0 else lax.ppermute(send, "member", pairs))
    send1, pick = call(
        late_kernel,
        [shape((GROUPS, LOCAL * CHUNKS[1], LAT), BF16), shape((tokens, tokens), BF16)],
        [HB] * 5,
        [VM, VM],
        state,
        flops=10**9,
        megabytes=16,
    )(order, member_seed, latents, perturbation, noise_table)
    got1 = lax.all_to_all(send1, "member", 0, 0, tiled=True)
    weights = tuple(far(w) for w in (w_gate, w_up, lowering_matrix))
    my_targets, *near = call(
        target_kernel,
        [pltpu.HBM((MINE, OUT), F32), *(shape(w.shape, BF16) for w in weights)],
        [SM] + [VM] * 5,
        [VM] * 4,
        flops=10**7,
        megabytes=10,
    )(me, pick, targets, *weights)
    my_targets = far(my_targets)
    earlier = call(
        first_kernel,
        pltpu.HBM((CHUNKS[0], LAT), F32),
        [HB] * GROUPS + [HB, VM, VM, VM],
        HB,
        (*scratch(CHUNKS[0]), pltpu.VMEM((MEMBERS * CHUNKS[0], LAT), BF16), pltpu.SemaphoreType.DMA((GROUPS,))),
        10**10,
        30,
    )(*(far(part) for part in got0), my_targets, *near)
    extra = (
        *scratch(CHUNKS[1]),
        pltpu.VMEM((LAT, HID), BF16),
        pltpu.VMEM((LAT, HID), BF16),
        pltpu.VMEM((HID, OUT), BF16),
        pltpu.SemaphoreType.DMA((3,)),
    )
    packed = call(last_kernel, shape((GROUPS, 16, 128), F32), [VM] + [HB] * 5, VM, extra, 5 * 10**9, 22)(
        got1.reshape(MEMBERS * CHUNKS[1], LAT), my_targets, *weights, far(earlier)
    )
    arrived = lax.all_to_all(packed, "member", 0, 0, tiled=True)
    columns = call(unpack_kernel, shape((LAT // GROUPS, tokens), F32), [VM] * 2, VM)(arrived, pick)
    return columns.T


def solution(mesh):
    in_specs = (
        P("space", None),
        P("member", "space", None),
        P(),
        P("member"),
        P(),
        P("space", None),
        P(),
        P(),
        P(),
    )
    return jax.shard_map(body, mesh=mesh, in_specs=in_specs, out_specs=P("space", "member"), check_vma=False)
```

```python
import jax
import jax.numpy as jnp
from jax import lax
from jax.experimental import pallas as pl
from jax.experimental.pallas import tpu as pltpu
from jax.sharding import PartitionSpec as P


LAT = 512
HID = 1024
OUT = 384
PIECE = 8
BLOCK = 384
PAD = 8
GROUPS = 16
MINE = 48
LOCAL = 3
MEMBERS = 48
Z = 8
OFFSETS = tuple((dz, dc) for dz in (3, 5, 4, 2, 6, 1, 7, 0) for dc in (0, 1))
CHUNKS = (32, 16)
STARTS = (0, 32)
SCALE = float(PIECE * OUT) ** 0.5
F32 = jnp.float32
BF16 = jnp.bfloat16
VM = pl.BlockSpec(memory_space=pltpu.VMEM)
SM = pl.BlockSpec(memory_space=pltpu.SMEM)
HB = pl.BlockSpec(memory_space=pltpu.HBM)


def far(x):
    return pltpu.with_memory_space_constraint(x, pltpu.HBM)


def dot(a, b):
    return jnp.dot(a, b, preferred_element_type=F32)


def dot_t(a, b):
    return lax.dot_general(a, b, (((1,), (1,)), ((), ())), preferred_element_type=F32)


def pieces(x):
    high = x.astype(BF16)
    rest = x - high.astype(F32)
    mid = rest.astype(BF16)
    low = (rest - mid.astype(F32)).astype(BF16)
    return high, mid, low


def columns_of(order):
    eye = lax.broadcasted_iota(jnp.int32, (128, 128), 0) == lax.broadcasted_iota(jnp.int32, (128, 128), 1)
    found = []
    for b in range(order.shape[0] // 128):
        row = order[pl.ds(128 * b, 128)].reshape(1, 128).astype(F32)
        found.append(jnp.sum(jnp.where(eye, row, 0.0), axis=1, keepdims=True).astype(jnp.int32))
    return found


def one_hot(columns, start, count, tokens):
    lane = lax.broadcasted_iota(jnp.int32, (16, tokens), 1)
    parts = []
    for d in range(GROUPS):
        for first in range(d * MINE + start, d * MINE + start + count, 16):
            column = columns[first // 128][first % 128 : first % 128 + 16]
            parts.append(jnp.where(column == lane, 1.0, 0.0).astype(BF16))
    return jnp.concatenate(parts, axis=0)


def move(noisy, picked, send, count):
    for m in range(LOCAL):
        moved = dot(picked, noisy(m)).astype(BF16)
        for d in range(GROUPS):
            send[d, m * count : (m + 1) * count, :] = moved[d * count : (d + 1) * count]


def load_state(order, seeds, latents, perturbation, table, order_here, seeds_here, latents_here, here, table_here, sems):
    first = pltpu.make_async_copy(order, order_here, sems.at[3 + LOCAL])
    first.start()
    copies = [
        pltpu.make_async_copy(seeds, seeds_here, sems.at[0]),
        pltpu.make_async_copy(table, table_here, sems.at[1]),
        pltpu.make_async_copy(latents, latents_here, sems.at[2]),
    ] + [pltpu.make_async_copy(perturbation.at[m], here.at[m], sems.at[3 + m]) for m in range(LOCAL)]
    for copy in copies:
        copy.start()
    first.wait()

    def noisy(m):
        if m == 0:
            for copy in copies[:3]:
                copy.wait()
        copies[3 + m].wait()
        factor = table_here[pl.ds(seeds_here[m], 1), :]
        return (latents_here[...].astype(F32) + here[m].astype(F32) * factor).astype(BF16)

    return noisy


def early_kernel(me, order, seeds, latents, perturbation, table, *rest):
    sends, state, pick = rest[:GROUPS], rest[GROUPS:-1], rest[-1]
    noisy = load_state(order, seeds, latents, perturbation, table, *state)
    count = CHUNKS[0]
    pick[...] = one_hot(columns_of(state[0]), STARTS[0], count, latents.shape[0])
    z, core = me[0] // 2, lax.rem(me[0], 2)
    parts = []
    for dz, dc in OFFSETS:
        there = lax.rem(z + dz, Z) * 2 + (1 - core if dc else core)
        parts.append(pick[pl.ds(pl.multiple_of(there * count, 16), count), :])
    picked = jnp.concatenate(parts, axis=0)
    for m in range(LOCAL):
        moved = dot(picked, noisy(m)).astype(BF16)
        for k, send in enumerate(sends):
            send[m * count : (m + 1) * count, :] = moved[k * count : (k + 1) * count]


def late_kernel(order, seeds, latents, perturbation, table, send, pick, *state):
    noisy = load_state(order, seeds, latents, perturbation, table, *state)
    columns = columns_of(state[0])
    pick[...] = one_hot(columns, 0, MINE, latents.shape[0])
    move(noisy, one_hot(columns, STARTS[1], CHUNKS[1], latents.shape[0]), send, CHUNKS[1])


def target_kernel(me, pick, targets, w_gate, w_up, lowering, my_targets, gate_here, up_here, low_here):
    my_targets[...] = dot(pick[pl.ds(pl.multiple_of(me[0] * MINE, 16), MINE), :], targets[...])
    gate_here[...] = w_gate[...]
    up_here[...] = w_up[...]
    low_here[...] = lowering[...]


def score(forecast, cotangent, target, p, gap_rows):
    def token(r):
        at = pl.ds(p * PIECE + r, MEMBERS, stride=gap_rows)
        u = jnp.concatenate([forecast[j, at, :] for j in range(3)], axis=1)
        return at, u, u - target[r : r + 1, :]

    gram = jnp.zeros((MEMBERS, MEMBERS), F32)
    norm = jnp.zeros((MEMBERS, 128), F32)
    for r in range(PIECE):
        at, u, miss = token(r)
        ub = u.astype(BF16)
        gram = gram + dot_t(ub, ub)
        square = miss * miss
        norm = norm + square[:, :128] + square[:, 128:256] + square[:, 256:]
    eye = lax.broadcasted_iota(jnp.int32, gram.shape, 0) == lax.broadcasted_iota(jnp.int32, gram.shape, 1)
    diagonal = jnp.where(eye, gram, 0.0)
    across = jnp.sum(diagonal, axis=1, keepdims=True)
    down = jnp.sum(diagonal, axis=0, keepdims=True)
    gap = across + down - 2.0 * gram
    weight = (1.0 / jnp.sqrt(jnp.where(eye, 0.0, gap) + 1.0)).astype(BF16)
    total = jnp.sum(weight.astype(F32), axis=1, keepdims=True)
    skill = SCALE / jnp.sqrt(jnp.sum(norm, axis=1, keepdims=True) + 1.0)
    for r in range(PIECE):
        at, u, miss = token(r)
        spread = (SCALE / MEMBERS * (total * u - dot(weight, u.astype(BF16)))).astype(BF16)
        made = skill * miss - spread.astype(F32)
        for j in range(3):
            cotangent[j, at, :] = made[:, 128 * j : 128 * j + 128]


def network(noisy, target, w_gate, w_up, lowering, state, count, start):
    left, right, forecast, cotangent, gate_sum, up_sum, target_here, sem = state[:8]
    copy = pltpu.make_async_copy(target.at[pl.ds(start, count)], target_here, sem)
    copy.start()
    total = MEMBERS * count
    block = BLOCK
    inside = block // count
    gap_rows = count + PAD

    @pl.loop(0, total // block)
    def _(i):
        at = pl.ds(pl.multiple_of(i * block, block), block)
        x = noisy[at, :]
        half = 0.5 * dot(x, w_gate[...])
        up = dot(x, w_up[...])
        bent = 1.0 + jnp.tanh(half)
        swish = half * bent
        s = 0.5 * bent
        right[at, :] = swish
        left[at, :] = up * (s + swish * (1.0 - s))
        made = dot((swish * up).astype(BF16), lowering[...]).astype(BF16).astype(F32)
        for q in range(inside):
            to = pl.ds(pl.multiple_of(i * inside * gap_rows + q * gap_rows, 8), count)
            for j in range(3):
                forecast[j, to, :] = made[count * q : count * q + count, 128 * j : 128 * j + 128]

    copy.wait()

    @pl.loop(0, count // PIECE)
    def _(p):
        score(forecast, cotangent, target_here[pl.ds(pl.multiple_of(p * PIECE, PIECE), PIECE), :], p, gap_rows)

    token = lax.broadcasted_iota(jnp.int32, (count, block), 0)
    place = lax.broadcasted_iota(jnp.int32, (count, block), 1)
    collect = jnp.where(lax.rem(place, count) == token, 1.0, 0.0).astype(BF16)
    gate_sum[...] = jnp.zeros((count, HID), F32)
    up_sum[...] = jnp.zeros((count, HID), F32)

    @pl.loop(0, total // block)
    def _(i):
        at = pl.ds(pl.multiple_of(i * block, block), block)
        rows = []
        for q in range(inside):
            back = pl.ds(pl.multiple_of(i * inside * gap_rows + q * gap_rows, 8), count)
            rows.append(jnp.concatenate([cotangent[j, back, :] for j in range(3)], axis=1))
        hidden_grad = dot_t(jnp.concatenate(rows, axis=0).astype(BF16), lowering[...])
        gate_sum[...] += dot(collect, (hidden_grad * left[at, :]).astype(BF16))
        up_sum[...] += dot(collect, (hidden_grad * right[at, :]).astype(BF16))

    gates = dot_t(jnp.concatenate(pieces(gate_sum[...]), axis=0), w_gate[...])
    ups = dot_t(jnp.concatenate(pieces(up_sum[...]), axis=0), w_up[...])
    both = gates + ups
    return both[:count] + both[count : 2 * count] + both[2 * count :]


def first_kernel(*refs):
    gathered, (target, w_gate, w_up, lowering, out), state = refs[:GROUPS], refs[GROUPS : GROUPS + 5], refs[GROUPS + 5 :]
    here, sem, noisy, sems = state[-4:]
    size = LOCAL * CHUNKS[0]
    copies = [
        pltpu.make_async_copy(part, noisy.at[pl.ds(k * size, size)], sems.at[k]) for k, part in enumerate(gathered)
    ]
    for copy in copies:
        copy.start()
    for copy in copies:
        copy.wait()
    here[...] = network(noisy, target, w_gate, w_up, lowering, state, CHUNKS[0], STARTS[0])
    copy = pltpu.make_async_copy(here, out, sem)
    copy.start()
    copy.wait()


def last_kernel(noisy, target, w_gate, w_up, lowering, earlier, out, *state):
    here, sem, gate_here, up_here, low_here, sems = state[-6:]
    copies = [
        pltpu.make_async_copy(w_gate, gate_here, sems.at[0]),
        pltpu.make_async_copy(w_up, up_here, sems.at[1]),
        pltpu.make_async_copy(lowering, low_here, sems.at[2]),
        pltpu.make_async_copy(earlier, here, sem),
    ]
    for copy in copies:
        copy.start()
    for copy in copies:
        copy.wait()
    grad = network(noisy, target, gate_here, up_here, low_here, state, CHUNKS[1], STARTS[1])
    parts = (here[:16], here[16:], grad)
    blank = jnp.zeros((16, 32), F32)
    for d in range(GROUPS):
        out[d] = jnp.concatenate([part[:, 32 * d : 32 * d + 32] for part in parts] + [blank], axis=1)


def unpack_kernel(arrived, pick, out):
    flat = arrived[...].reshape(GROUPS * 16, 128)
    turned = flat.T
    total = jnp.zeros(out.shape, F32)
    for c in range(3):
        rows = jnp.concatenate([pick[d * MINE + 16 * c : d * MINE + 16 * c + 16, :] for d in range(GROUPS)], axis=0)
        placed = dot(jnp.concatenate(pieces(turned[32 * c : 32 * c + 32]), axis=0), rows)
        total = total + placed[:32] + placed[32:64] + placed[64:]
    out[...] = total


def call(kernel, out_shape, specs, out_specs, scratch=(), flops=0, megabytes=24):
    return pl.pallas_call(
        kernel,
        out_shape=out_shape,
        in_specs=specs,
        out_specs=out_specs,
        scratch_shapes=list(scratch),
        compiler_params=pltpu.CompilerParams(vmem_limit_bytes=megabytes * 1024 * 1024),
        cost_estimate=pl.CostEstimate(flops=flops, transcendentals=0, bytes_accessed=0) if flops else None,
    )


def scratch(count):
    rows = MEMBERS * count
    padded = MEMBERS * (count + PAD)
    return (
        pltpu.VMEM((rows, HID), F32),
        pltpu.VMEM((rows, HID), F32),
        pltpu.VMEM((3, padded, 128), F32),
        pltpu.VMEM((3, padded, 128), F32),
        pltpu.VMEM((count, HID), F32),
        pltpu.VMEM((count, HID), F32),
        pltpu.VMEM((count, OUT), F32),
        pltpu.SemaphoreType.DMA,
        pltpu.VMEM((CHUNKS[0], LAT), F32),
        pltpu.SemaphoreType.DMA,
    )


def body(latents, perturbation, noise_table, member_seed, piece_arrangement, targets, w_gate, w_up, lowering_matrix):
    tokens = latents.shape[0]
    latents, perturbation, noise_table, member_seed, targets = (
        far(x) for x in (latents, perturbation, noise_table, member_seed, targets)
    )
    me = lax.axis_index("member").astype(jnp.int32).reshape(1)
    shape = jax.ShapeDtypeStruct
    order = far(piece_arrangement)
    state = (
        pltpu.VMEM((tokens,), jnp.int32),
        pltpu.SMEM((LOCAL,), jnp.int32),
        pltpu.VMEM((tokens, LAT), BF16),
        pltpu.VMEM((LOCAL, tokens, LAT), BF16),
        pltpu.VMEM(noise_table.shape, F32),
        pltpu.SemaphoreType.DMA((4 + LOCAL,)),
    )
    sends = call(
        early_kernel,
        [(shape if any(o) else pltpu.HBM)((LOCAL * CHUNKS[0], LAT), BF16) for o in OFFSETS],
        [SM] + [HB] * 5,
        [VM] * GROUPS,
        (*state, pltpu.VMEM((GROUPS * CHUNKS[0], tokens), BF16)),
        megabytes=16,
    )(me, order, member_seed, latents, perturbation, noise_table)
    got0 = []
    for (dz, dc), send in zip(OFFSETS, sends):
        pairs = [(2 * z + c, (z + dz) % Z * 2 + (c ^ dc)) for z in range(Z) for c in range(2)]
        got0.append(send if dz == dc == 0 else lax.ppermute(send, "member", pairs))
    send1, pick = call(
        late_kernel,
        [shape((GROUPS, LOCAL * CHUNKS[1], LAT), BF16), shape((tokens, tokens), BF16)],
        [HB] * 5,
        [VM, VM],
        state,
        flops=10**9,
        megabytes=16,
    )(order, member_seed, latents, perturbation, noise_table)
    got1 = lax.all_to_all(send1, "member", 0, 0, tiled=True)
    weights = tuple(far(w) for w in (w_gate, w_up, lowering_matrix))
    my_targets, *near = call(
        target_kernel,
        [pltpu.HBM((MINE, OUT), F32), *(shape(w.shape, BF16) for w in weights)],
        [SM] + [VM] * 5,
        [VM] * 4,
        flops=10**7,
        megabytes=10,
    )(me, pick, targets, *weights)
    my_targets = far(my_targets)
    earlier = call(
        first_kernel,
        pltpu.HBM((CHUNKS[0], LAT), F32),
        [HB] * GROUPS + [HB, VM, VM, VM],
        HB,
        (*scratch(CHUNKS[0]), pltpu.VMEM((MEMBERS * CHUNKS[0], LAT), BF16), pltpu.SemaphoreType.DMA((GROUPS,))),
        10**10,
        30,
    )(*(far(part) for part in got0), my_targets, *near)
    extra = (
        *scratch(CHUNKS[1]),
        pltpu.VMEM((LAT, HID), BF16),
        pltpu.VMEM((LAT, HID), BF16),
        pltpu.VMEM((HID, OUT), BF16),
        pltpu.SemaphoreType.DMA((3,)),
    )
    packed = call(last_kernel, shape((GROUPS, 16, 128), F32), [VM] + [HB] * 5, VM, extra, 5 * 10**9, 22)(
        got1.reshape(MEMBERS * CHUNKS[1], LAT), my_targets, *weights, far(earlier)
    )
    arrived = lax.all_to_all(packed, "member", 0, 0, tiled=True)
    columns = call(unpack_kernel, shape((LAT // GROUPS, tokens), F32), [VM] * 2, VM)(arrived, pick)
    return columns.T


def solution(mesh):
    in_specs = (
        P("space", None),
        P("member", "space", None),
        P(),
        P("member"),
        P(),
        P("space", None),
        P(),
        P(),
        P(),
    )
    return jax.shard_map(body, mesh=mesh, in_specs=in_specs, out_specs=P("space", "member"), check_vma=False)
```

```python
import jax
import jax.numpy as jnp
from jax import lax
from jax.experimental import pallas as pl
from jax.experimental.pallas import tpu as pltpu
from jax.sharding import PartitionSpec as P


LAT = 512
HID = 1024
OUT = 384
PIECE = 8
BLOCK = 384
PAD = 8
GROUPS = 16
MINE = 48
LOCAL = 3
MEMBERS = 48
Z = 8
OFFSETS = (
    *((1, 0), (7, 0), (3, 0), (5, 0), (4, 0), (4, 1), (3, 1), (5, 1)),
    *((2, 0), (6, 0), (2, 1), (6, 1), (1, 1), (7, 1), (0, 1), (0, 0)),
)
CHUNKS = (32, 16)
STARTS = (0, 32)
SCALE = float(PIECE * OUT) ** 0.5
F32 = jnp.float32
BF16 = jnp.bfloat16
VM = pl.BlockSpec(memory_space=pltpu.VMEM)
SM = pl.BlockSpec(memory_space=pltpu.SMEM)
HB = pl.BlockSpec(memory_space=pltpu.HBM)


def far(x):
    return pltpu.with_memory_space_constraint(x, pltpu.HBM)


def dot(a, b):
    return jnp.dot(a, b, preferred_element_type=F32)


def dot_t(a, b):
    return lax.dot_general(a, b, (((1,), (1,)), ((), ())), preferred_element_type=F32)


def pieces(x):
    high = x.astype(BF16)
    rest = x - high.astype(F32)
    mid = rest.astype(BF16)
    low = (rest - mid.astype(F32)).astype(BF16)
    return high, mid, low


def columns_of(order):
    eye = lax.broadcasted_iota(jnp.int32, (128, 128), 0) == lax.broadcasted_iota(jnp.int32, (128, 128), 1)
    found = []
    for b in range(order.shape[0] // 128):
        row = order[pl.ds(128 * b, 128)].reshape(1, 128).astype(F32)
        found.append(jnp.sum(jnp.where(eye, row, 0.0), axis=1, keepdims=True).astype(jnp.int32))
    return found


def one_hot(columns, start, count, tokens):
    lane = lax.broadcasted_iota(jnp.int32, (16, tokens), 1)
    parts = []
    for d in range(GROUPS):
        for first in range(d * MINE + start, d * MINE + start + count, 16):
            column = columns[first // 128][first % 128 : first % 128 + 16]
            parts.append(jnp.where(column == lane, 1.0, 0.0).astype(BF16))
    return jnp.concatenate(parts, axis=0)


def move(noisy, picked, send, count):
    for m in range(LOCAL):
        moved = dot(picked, noisy(m)).astype(BF16)
        for d in range(GROUPS):
            send[d, m * count : (m + 1) * count, :] = moved[d * count : (d + 1) * count]


def load_state(order, seeds, latents, perturbation, table, order_here, seeds_here, latents_here, here, table_here, sems):
    first = pltpu.make_async_copy(order, order_here, sems.at[3 + LOCAL])
    first.start()
    copies = [
        pltpu.make_async_copy(seeds, seeds_here, sems.at[0]),
        pltpu.make_async_copy(table, table_here, sems.at[1]),
        pltpu.make_async_copy(latents, latents_here, sems.at[2]),
    ] + [pltpu.make_async_copy(perturbation.at[m], here.at[m], sems.at[3 + m]) for m in range(LOCAL)]
    for copy in copies:
        copy.start()
    first.wait()

    def noisy(m):
        if m == 0:
            for copy in copies[:3]:
                copy.wait()
        copies[3 + m].wait()
        factor = table_here[pl.ds(seeds_here[m], 1), :]
        return (latents_here[...].astype(F32) + here[m].astype(F32) * factor).astype(BF16)

    return noisy


def early_kernel(me, order, seeds, latents, perturbation, table, *rest):
    sends, state, pick = rest[:GROUPS], rest[GROUPS:-1], rest[-1]
    noisy = load_state(order, seeds, latents, perturbation, table, *state)
    count = CHUNKS[0]
    pick[...] = one_hot(columns_of(state[0]), STARTS[0], count, latents.shape[0])
    z, core = me[0] // 2, lax.rem(me[0], 2)
    parts = []
    for dz, dc in OFFSETS:
        there = lax.rem(z + dz, Z) * 2 + (1 - core if dc else core)
        parts.append(pick[pl.ds(pl.multiple_of(there * count, 16), count), :])
    picked = jnp.concatenate(parts, axis=0)
    for m in range(LOCAL):
        moved = dot(picked, noisy(m)).astype(BF16)
        for k, send in enumerate(sends):
            send[m * count : (m + 1) * count, :] = moved[k * count : (k + 1) * count]


def late_kernel(order, seeds, latents, perturbation, table, send, pick, *state):
    noisy = load_state(order, seeds, latents, perturbation, table, *state)
    columns = columns_of(state[0])
    pick[...] = one_hot(columns, 0, MINE, latents.shape[0])
    move(noisy, one_hot(columns, STARTS[1], CHUNKS[1], latents.shape[0]), send, CHUNKS[1])


def target_kernel(me, pick, targets, w_gate, w_up, lowering, my_targets, gate_here, up_here, low_here):
    my_targets[...] = dot(pick[pl.ds(pl.multiple_of(me[0] * MINE, 16), MINE), :], targets[...])
    gate_here[...] = w_gate[...]
    up_here[...] = w_up[...]
    low_here[...] = lowering[...]


def score(forecast, cotangent, target, p, gap_rows):
    def token(r):
        at = pl.ds(p * PIECE + r, MEMBERS, stride=gap_rows)
        u = jnp.concatenate([forecast[j, at, :] for j in range(3)], axis=1)
        return at, u, u - target[r : r + 1, :]

    gram = jnp.zeros((MEMBERS, MEMBERS), F32)
    norm = jnp.zeros((MEMBERS, 128), F32)
    for r in range(PIECE):
        at, u, miss = token(r)
        ub = u.astype(BF16)
        gram = gram + dot_t(ub, ub)
        square = miss * miss
        norm = norm + square[:, :128] + square[:, 128:256] + square[:, 256:]
    eye = lax.broadcasted_iota(jnp.int32, gram.shape, 0) == lax.broadcasted_iota(jnp.int32, gram.shape, 1)
    diagonal = jnp.where(eye, gram, 0.0)
    across = jnp.sum(diagonal, axis=1, keepdims=True)
    down = jnp.sum(diagonal, axis=0, keepdims=True)
    gap = across + down - 2.0 * gram
    weight = (1.0 / jnp.sqrt(jnp.where(eye, 0.0, gap) + 1.0)).astype(BF16)
    total = jnp.sum(weight.astype(F32), axis=1, keepdims=True)
    skill = SCALE / jnp.sqrt(jnp.sum(norm, axis=1, keepdims=True) + 1.0)
    for r in range(PIECE):
        at, u, miss = token(r)
        spread = (SCALE / MEMBERS * (total * u - dot(weight, u.astype(BF16)))).astype(BF16)
        made = skill * miss - spread.astype(F32)
        for j in range(3):
            cotangent[j, at, :] = made[:, 128 * j : 128 * j + 128]


def network(noisy, target, w_gate, w_up, lowering, state, count, start, pending=()):
    left, right, forecast, cotangent, gate_sum, up_sum, target_here, sem = state[:8]
    copy = pltpu.make_async_copy(target.at[pl.ds(start, count)], target_here, sem)
    copy.start()
    total = MEMBERS * count
    block = BLOCK
    inside = block // count
    gap_rows = count + PAD

    def forward(i, pending=()):
        known = isinstance(i, int)
        at = pl.ds(i * block if known else pl.multiple_of(i * block, block), block)
        x = noisy[at, :]
        for late in pending[:1]:
            late.wait()
        half = 0.5 * dot(x, w_gate[...])
        for late in pending[1:2]:
            late.wait()
        up = dot(x, w_up[...])
        bent = 1.0 + jnp.tanh(half)
        swish = half * bent
        s = 0.5 * bent
        right[at, :] = swish
        left[at, :] = up * (s + swish * (1.0 - s))
        for late in pending[2:]:
            late.wait()
        made = dot((swish * up).astype(BF16), lowering[...]).astype(BF16).astype(F32)
        for q in range(inside):
            to = i * inside * gap_rows + q * gap_rows
            to = pl.ds(to if known else pl.multiple_of(to, 8), count)
            for j in range(3):
                forecast[j, to, :] = made[count * q : count * q + count, 128 * j : 128 * j + 128]

    if pending:
        for i in range(total // block):
            forward(i, () if i else pending)
    else:
        pl.loop(0, total // block)(forward)

    copy.wait()

    @pl.loop(0, count // PIECE)
    def _(p):
        score(forecast, cotangent, target_here[pl.ds(pl.multiple_of(p * PIECE, PIECE), PIECE), :], p, gap_rows)

    token = lax.broadcasted_iota(jnp.int32, (count, block), 0)
    place = lax.broadcasted_iota(jnp.int32, (count, block), 1)
    collect = jnp.where(lax.rem(place, count) == token, 1.0, 0.0).astype(BF16)
    gate_sum[...] = jnp.zeros((count, HID), F32)
    up_sum[...] = jnp.zeros((count, HID), F32)

    @pl.loop(0, total // block)
    def _(i):
        at = pl.ds(pl.multiple_of(i * block, block), block)
        rows = []
        for q in range(inside):
            back = pl.ds(pl.multiple_of(i * inside * gap_rows + q * gap_rows, 8), count)
            rows.append(jnp.concatenate([cotangent[j, back, :] for j in range(3)], axis=1))
        hidden_grad = dot_t(jnp.concatenate(rows, axis=0).astype(BF16), lowering[...])
        gate_sum[...] += dot(collect, (hidden_grad * left[at, :]).astype(BF16))
        up_sum[...] += dot(collect, (hidden_grad * right[at, :]).astype(BF16))

    gates = dot_t(jnp.concatenate(pieces(gate_sum[...]), axis=0), w_gate[...])
    ups = dot_t(jnp.concatenate(pieces(up_sum[...]), axis=0), w_up[...])
    both = gates + ups
    return both[:count] + both[count : 2 * count] + both[2 * count :]


def first_kernel(*refs):
    gathered, (target, w_gate, w_up, lowering, out), state = refs[:GROUPS], refs[GROUPS : GROUPS + 5], refs[GROUPS + 5 :]
    here, sem, noisy, sems = state[-4:]
    size = LOCAL * CHUNKS[0]
    copies = [
        pltpu.make_async_copy(part, noisy.at[pl.ds(k * size, size)], sems.at[k]) for k, part in enumerate(gathered)
    ]
    for copy in copies:
        copy.start()
    for copy in copies:
        copy.wait()
    here[...] = network(noisy, target, w_gate, w_up, lowering, state, CHUNKS[0], STARTS[0])
    copy = pltpu.make_async_copy(here, out, sem)
    copy.start()
    copy.wait()


def last_kernel(noisy, target, w_gate, w_up, lowering, earlier, out, *state):
    here, sem, gate_here, up_here, low_here, sems = state[-6:]
    copies = [
        pltpu.make_async_copy(w_gate, gate_here, sems.at[0]),
        pltpu.make_async_copy(w_up, up_here, sems.at[1]),
        pltpu.make_async_copy(lowering, low_here, sems.at[2]),
        pltpu.make_async_copy(earlier, here, sem),
    ]
    for copy in copies:
        copy.start()
    grad = network(
        noisy, target, gate_here, up_here, low_here, state, CHUNKS[1], STARTS[1], (copies[0], copies[1], copies[2])
    )
    copies[3].wait()
    parts = (here[:16], here[16:], grad)
    blank = jnp.zeros((16, 32), F32)
    for d in range(GROUPS):
        out[d] = jnp.concatenate([part[:, 32 * d : 32 * d + 32] for part in parts] + [blank], axis=1)


def unpack_kernel(arrived, pick, out):
    flat = arrived[...].reshape(GROUPS * 16, 128)
    turned = flat.T
    total = jnp.zeros(out.shape, F32)
    for c in range(3):
        rows = jnp.concatenate([pick[d * MINE + 16 * c : d * MINE + 16 * c + 16, :] for d in range(GROUPS)], axis=0)
        placed = dot(jnp.concatenate(pieces(turned[32 * c : 32 * c + 32]), axis=0), rows)
        total = total + placed[:32] + placed[32:64] + placed[64:]
    out[...] = total


def call(kernel, out_shape, specs, out_specs, scratch=(), flops=0, megabytes=24):
    return pl.pallas_call(
        kernel,
        out_shape=out_shape,
        in_specs=specs,
        out_specs=out_specs,
        scratch_shapes=list(scratch),
        compiler_params=pltpu.CompilerParams(vmem_limit_bytes=megabytes * 1024 * 1024),
        cost_estimate=pl.CostEstimate(flops=flops, transcendentals=0, bytes_accessed=0) if flops else None,
    )


def scratch(count):
    rows = MEMBERS * count
    padded = MEMBERS * (count + PAD)
    return (
        pltpu.VMEM((rows, HID), F32),
        pltpu.VMEM((rows, HID), F32),
        pltpu.VMEM((3, padded, 128), F32),
        pltpu.VMEM((3, padded, 128), F32),
        pltpu.VMEM((count, HID), F32),
        pltpu.VMEM((count, HID), F32),
        pltpu.VMEM((count, OUT), F32),
        pltpu.SemaphoreType.DMA,
        pltpu.VMEM((CHUNKS[0], LAT), F32),
        pltpu.SemaphoreType.DMA,
    )


def body(latents, perturbation, noise_table, member_seed, piece_arrangement, targets, w_gate, w_up, lowering_matrix):
    tokens = latents.shape[0]
    latents, perturbation, noise_table, member_seed, targets = (
        far(x) for x in (latents, perturbation, noise_table, member_seed, targets)
    )
    me = lax.axis_index("member").astype(jnp.int32).reshape(1)
    shape = jax.ShapeDtypeStruct
    order = far(piece_arrangement)
    state = (
        pltpu.VMEM((tokens,), jnp.int32),
        pltpu.SMEM((LOCAL,), jnp.int32),
        pltpu.VMEM((tokens, LAT), BF16),
        pltpu.VMEM((LOCAL, tokens, LAT), BF16),
        pltpu.VMEM(noise_table.shape, F32),
        pltpu.SemaphoreType.DMA((4 + LOCAL,)),
    )
    sends = call(
        early_kernel,
        [(shape if any(o) else pltpu.HBM)((LOCAL * CHUNKS[0], LAT), BF16) for o in OFFSETS],
        [SM] + [HB] * 5,
        [VM] * GROUPS,
        (*state, pltpu.VMEM((GROUPS * CHUNKS[0], tokens), BF16)),
        megabytes=16,
    )(me, order, member_seed, latents, perturbation, noise_table)
    got0 = []
    for (dz, dc), send in zip(OFFSETS, sends):
        pairs = [(2 * z + c, (z + dz) % Z * 2 + (c ^ dc)) for z in range(Z) for c in range(2)]
        got0.append(send if dz == dc == 0 else lax.ppermute(send, "member", pairs))
    send1, pick = call(
        late_kernel,
        [shape((GROUPS, LOCAL * CHUNKS[1], LAT), BF16), shape((tokens, tokens), BF16)],
        [HB] * 5,
        [VM, VM],
        state,
        flops=10**9,
        megabytes=16,
    )(order, member_seed, latents, perturbation, noise_table)
    got1 = lax.all_to_all(send1, "member", 0, 0, tiled=True)
    weights = tuple(far(w) for w in (w_gate, w_up, lowering_matrix))
    my_targets, *near = call(
        target_kernel,
        [pltpu.HBM((MINE, OUT), F32), *(shape(w.shape, BF16) for w in weights)],
        [SM] + [VM] * 5,
        [VM] * 4,
        flops=10**7,
        megabytes=10,
    )(me, pick, targets, *weights)
    my_targets = far(my_targets)
    earlier = call(
        first_kernel,
        pltpu.HBM((CHUNKS[0], LAT), F32),
        [HB] * GROUPS + [HB, VM, VM, VM],
        HB,
        (*scratch(CHUNKS[0]), pltpu.VMEM((MEMBERS * CHUNKS[0], LAT), BF16), pltpu.SemaphoreType.DMA((GROUPS,))),
        10**10,
        30,
    )(*(far(part) for part in got0), my_targets, *near)
    extra = (
        *scratch(CHUNKS[1]),
        pltpu.VMEM((LAT, HID), BF16),
        pltpu.VMEM((LAT, HID), BF16),
        pltpu.VMEM((HID, OUT), BF16),
        pltpu.SemaphoreType.DMA((3,)),
    )
    packed = call(last_kernel, shape((GROUPS, 16, 128), F32), [VM] + [HB] * 5, VM, extra, 5 * 10**9, 22)(
        got1.reshape(MEMBERS * CHUNKS[1], LAT), my_targets, *weights, far(earlier)
    )
    arrived = lax.all_to_all(packed, "member", 0, 0, tiled=True)
    columns = call(unpack_kernel, shape((LAT // GROUPS, tokens), F32), [VM] * 2, VM)(arrived, pick)
    return columns.T


def solution(mesh):
    in_specs = (
        P("space", None),
        P("member", "space", None),
        P(),
        P("member"),
        P(),
        P("space", None),
        P(),
        P(),
        P(),
    )
    return jax.shard_map(body, mesh=mesh, in_specs=in_specs, out_specs=P("space", "member"), check_vma=False)
```
